32 devices in a mesh: dp: 4 (over y, z), tp: 8 (over x, core).
Axes of the slice: x: 4, y: 2, z: 2, core: 2. Of those that a mesh axis runs over, the one named last changes fastest.
The devices are a block of a 4x4x8 slice.
Arguments:
- hidden: bfloat16 [65536, 1024], P(('dp', 'tp')), parts along dimension 0
- ln_gain: float32 [1024], replicated
- ln_bias: float32 [1024], replicated
- embed: bfloat16 [8192, 1024], P('tp')
- targets: int32 [65536], P(('dp', 'tp')), parts along dimension 0
- loss_mask: int32 [65536], P(('dp', 'tp')), parts along dimension 0
Outputs:
- output 1: float32 [65536], P(('dp', 'tp')), parts along dimension 0
- output 2: float32 [4], P('dp'), parts along dimension 0
- output 3: bfloat16 [65536, 1024], P(('dp', 'tp')), parts along dimension 0
- output 4: float32 [32768, 1024], P(('dp', 'tp')), parts along dimension 0
- output 5: float32 [4096], P('dp'), parts along dimension 0
- output 6: float32 [4096], P('dp'), parts along dimension 0
There are 4 independent parts. The reference program is written for one: setup_inputs(seed, part) draws one part's arguments, and reference() takes and returns one part's arrays. A program takes and returns all parts, laid end to end along the dimension named above; an argument that names none is the same for every part.
All inputs are finite; a program needn't handle non-finite values.
Results may differ from the reference program's by a relative error of at most 0.001.
Values are sent between devices in bfloat16 or wider.
A program may use at most 768 MiB of HBM per device.

```python
import jax
import jax.numpy as jnp
from jax import lax

TOKENS_DEV = 2048
GROUP_SIZE = 8
MODEL_DIM = 1024
VOCAB_SIZE = 8192
LN_EPS = 1e-5


def setup_inputs(seed: int = 0, part: int = 0) -> dict:
    seq_len = GROUP_SIZE * TOKENS_DEV
    part_keys = jax.random.split(jax.random.fold_in(jax.random.key(seed), part), 4)
    shared_keys = jax.random.split(jax.random.key(seed + 1), 3)
    embed_scale = 2.5 * MODEL_DIM ** -0.5
    hidden = jax.random.normal(part_keys[0], (seq_len, MODEL_DIM), jnp.float32).astype(jnp.bfloat16)
    ln_gain = 1.0 + 0.3 * jax.random.normal(shared_keys[0], (MODEL_DIM,), jnp.float32)
    ln_bias = 0.3 * jax.random.normal(shared_keys[1], (MODEL_DIM,), jnp.float32)
    embed = (embed_scale * jax.random.normal(shared_keys[2], (VOCAB_SIZE, MODEL_DIM), jnp.float32)).astype(jnp.bfloat16)
    targets = jax.random.randint(part_keys[1], (seq_len,), 0, VOCAB_SIZE, dtype=jnp.int32)
    shard_rate = jax.random.randint(part_keys[2], (GROUP_SIZE, 1), 40, 96, dtype=jnp.int32)
    draws = jax.random.randint(part_keys[3], (GROUP_SIZE, TOKENS_DEV), 0, 100, dtype=jnp.int32)
    loss_mask = (draws < shard_rate).astype(jnp.int32).reshape(seq_len)
    return {'hidden': hidden, 'ln_gain': ln_gain, 'ln_bias': ln_bias, 'embed': embed, 'targets': targets, 'loss_mask': loss_mask}


def normalize(hidden):
    h_f32 = hidden.astype(jnp.float32)
    centred = h_f32 - jnp.mean(h_f32, axis=-1, keepdims=True)
    inv_std = lax.rsqrt(jnp.mean(centred * centred, axis=-1, keepdims=True) + LN_EPS)
    return centred * inv_std, inv_std


def reference(hidden, ln_gain, ln_bias, embed, targets, loss_mask):
    seq_len = GROUP_SIZE * TOKENS_DEV
    x_hat, inv_std = normalize(hidden)
    normed = (x_hat * ln_gain + ln_bias).astype(jnp.bfloat16)
    weights = loss_mask.astype(jnp.float32)
    count = jnp.sum(weights)
    vocab_ids = jnp.arange(VOCAB_SIZE, dtype=jnp.int32)

    def block_step(embed_acc, block):
        x_blk, t_blk, w_blk = block
        logits = jnp.dot(x_blk, embed.T, preferred_element_type=jnp.float32)
        row_max = jnp.max(logits, axis=-1, keepdims=True)
        log_norm = row_max[:, 0] + jnp.log(jnp.sum(jnp.exp(logits - row_max), axis=-1))
        onehot = (vocab_ids[None, :] == t_blk[:, None]).astype(jnp.float32)
        t_logit = jnp.sum(logits * onehot, axis=-1)
        loss_blk = (log_norm - t_logit) * w_blk
        d_logits = ((jnp.exp(logits - log_norm[:, None]) - onehot) * (w_blk / count)[:, None]).astype(jnp.bfloat16)
        embed_acc = embed_acc + jnp.dot(d_logits.T, x_blk, preferred_element_type=jnp.float32)
        d_x = jnp.dot(d_logits, embed, preferred_element_type=jnp.float32)
        return embed_acc, (loss_blk, d_x)

    blocks = (normed.reshape(GROUP_SIZE, TOKENS_DEV, MODEL_DIM), targets.reshape(GROUP_SIZE, TOKENS_DEV), weights.reshape(GROUP_SIZE, TOKENS_DEV))
    d_embed, outs = lax.scan(block_step, jnp.zeros((VOCAB_SIZE, MODEL_DIM), jnp.float32), blocks)
    loss = outs[0].reshape(seq_len)
    d_normed = outs[1].reshape(seq_len, MODEL_DIM)
    mean_loss = jnp.sum(loss) / count
    d_gain = jnp.sum(d_normed * x_hat, axis=0)
    d_bias = jnp.sum(d_normed, axis=0)
    d_xhat = d_normed * ln_gain
    centre_term = jnp.mean(d_xhat, axis=-1, keepdims=True)
    proj_term = jnp.mean(d_xhat * x_hat, axis=-1, keepdims=True)
    d_hidden = (inv_std * (d_xhat - centre_term - x_hat * proj_term)).astype(jnp.bfloat16)
    return loss, mean_loss.reshape(1), d_hidden, d_embed, d_gain, d_bias
```

```python
import jax
import jax.numpy as jnp
from jax import lax
from jax.sharding import PartitionSpec as P

LN_EPS = 1e-5


def layer_norm(hidden, ln_gain, ln_bias):
    h_f32 = hidden.astype(jnp.float32)
    centred = h_f32 - jnp.mean(h_f32, axis=-1, keepdims=True)
    inv_std = lax.rsqrt(jnp.mean(centred * centred, axis=-1, keepdims=True) + LN_EPS)
    x_hat = centred * inv_std
    return x_hat, inv_std, (x_hat * ln_gain + ln_bias).astype(jnp.bfloat16)


def norm_backward(d_normed, x_hat, inv_std, ln_gain):
    scaled = d_normed * ln_gain
    centre_term = jnp.mean(scaled, axis=-1, keepdims=True)
    proj_term = jnp.mean(scaled * x_hat, axis=-1, keepdims=True)
    return (inv_std * (scaled - centre_term - x_hat * proj_term)).astype(jnp.bfloat16)


def solution(mesh):
    def body(hidden, ln_gain, ln_bias, embed, targets, loss_mask):
        table = lax.all_gather(embed, 'tp', tiled=True)
        weights = loss_mask.astype(jnp.float32)
        count = lax.psum(jnp.sum(weights), 'tp')
        x_hat, inv_std, normed = layer_norm(hidden, ln_gain, ln_bias)
        logits = jnp.einsum('sd,vd->sv', normed, table, preferred_element_type=jnp.float32)
        onehot = lax.broadcasted_iota(jnp.int32, (1, table.shape[0]), 1) == targets[:, None]
        row_max = jnp.max(logits, axis=-1)
        row_sum = jnp.sum(jnp.exp(logits - row_max[:, None]), axis=-1)
        t_logit = jnp.sum(jnp.where(onehot, logits, 0.0), axis=-1)
        log_norm = row_max + jnp.log(row_sum)
        loss = (log_norm - t_logit) * weights
        d_logits = ((jnp.exp(logits - log_norm[:, None]) - onehot.astype(jnp.float32)) * (weights / count)[:, None]).astype(jnp.bfloat16)
        d_embed_part = jnp.einsum('sv,sd->vd', d_logits, normed, preferred_element_type=jnp.float32)
        d_embed = lax.psum_scatter(d_embed_part, 'tp', scatter_dimension=0, tiled=True)
        d_normed = jnp.einsum('sv,vd->sd', d_logits, table, preferred_element_type=jnp.float32)
        sums = jnp.concatenate([jnp.sum(d_normed * x_hat, axis=0), jnp.sum(d_normed, axis=0), jnp.full((128,), jnp.sum(loss))])
        sums = lax.psum(sums, 'tp')
        dim = hidden.shape[1]
        mean_loss = sums[2 * dim:2 * dim + 1] / count
        d_hidden = norm_backward(d_normed, x_hat, inv_std, ln_gain)
        return loss, mean_loss, d_hidden, d_embed, sums[:dim], sums[dim:2 * dim]

    token_rows = P(('dp', 'tp'))
    token_mat = P(('dp', 'tp'), None)
    return jax.shard_map(body, mesh=mesh, in_specs=(token_mat, P(), P(), P('tp', None), token_rows, token_rows), out_specs=(token_rows, P('dp'), token_mat, token_mat, P('dp'), P('dp')), check_vma=False)
```

```python
import functools

import jax
import jax.numpy as jnp
from jax import lax
from jax.experimental import pallas as pl
from jax.experimental.pallas import tpu as pltpu
from jax.sharding import PartitionSpec as P

LN_EPS = 1e-5
LANES = 128
PIECE = 256
TILE = 512
MESH = pl.DeviceIdType.MESH
F32 = jnp.float32
BF16 = jnp.bfloat16


def matmul_t(a, b):
    return lax.dot_general(a, b, (((1,), (1,)), ((), ())), preferred_element_type=F32)


def matmul(a, b):
    return jnp.dot(a, b, preferred_element_type=F32)


def widen(col, width):
    return jnp.concatenate([col] * (width // LANES), axis=1)


def to_row(col):
    return jnp.transpose(jnp.broadcast_to(col, (LANES, LANES)))[0:1, :]


def to_col(row):
    return jnp.transpose(jnp.broadcast_to(row, (LANES, LANES)))


def kernel(n, hidden, gain, bias, embed, tgt, msk,
           loss_o, mean_o, dh_o, de_o, dg_o, db_o, z_h, x_h,
           e_all, x_own, hid, de_acc, max_s, sum_s, mu_s, rs_s, xbuf, dz_a, dz_b, zb, dx_acc, zt,
           tcol, wcol, tg_all, mk_all, ls_all, sm_all, gb, inv_s,
           e_send, e_recv, ep_send, ep_recv, e_pair, x_send, x_recv, xp_send, xp_recv, x_pair,
           tg_sem, mk_sem, ls_sem, sm_sem, hid_sem, loc_sem, z_sem, zl_sem, xl_sem, dh_sem):
    tokens, dim = hid.shape
    shard = embed.shape[0]
    chips = n // 2
    e_parts, x_parts = shard // PIECE, tokens // PIECE
    e_rounds, x_rounds = e_parts + e_parts // 2, x_parts + x_parts // 2
    blocks = tokens // LANES
    tiles = tokens // TILE
    me = lax.axis_index('tp')
    chip, core = me // 2, me % 2
    partner = 2 * chip + 1 - core
    right, left = (me + 2) % n, (me + n - 2) % n
    ring_dev = (right, left)

    def remote(src, dst, ssem, rsem, dev):
        return pltpu.make_async_remote_copy(src_ref=src, dst_ref=dst, send_sem=ssem, recv_sem=rsem,
                                            device_id={'tp': dev}, device_id_type=MESH)

    def piece(buf, slot, q):
        return buf.at[slot, pl.ds(pl.multiple_of(q * PIECE, PIECE), PIECE), :]

    def ring_src(j, d, parts):
        off = (2 * d - 1) * (j // parts)
        return 2 * ((chip + off + chips) % chips) + core, (j + d * (parts // 2)) % parts

    def arrival(j, d, parts, lane):
        off = (2 * d - 1) * (1 + j // parts)
        side = core + lane * (1 - 2 * core)
        return 2 * ((chip + off + chips) % chips) + side, (j + d * (parts // 2)) % parts

    def e_ring(j, d, src=None):
        slot, q = ring_src(j, d, e_parts)
        ref = piece(e_all, slot, q)
        if src is None:
            src = ref
        else:
            src = src.at[pl.ds(pl.multiple_of(q * PIECE, PIECE), PIECE), :]
        return remote(src, ref, e_send.at[d, j], e_recv.at[d, j], ring_dev[d])

    def e_relay(j, d, lane):
        slot, q = arrival(j, d, e_parts, lane)
        ref = piece(e_all, slot, q)
        return remote(ref, ref, ep_send.at[d, j], ep_recv.at[d, j], partner)

    def e_wait(j, d):
        slot, q = arrival(j, d, e_parts, 0)
        ref = piece(e_all, slot, q)
        remote(ref, ref, e_send.at[d, j], e_recv.at[d, j], ring_dev[d]).wait_recv()

    def x_ring(j, d):
        slot, q = ring_src(j, d, x_parts)
        ref = piece(x_h, slot, q)
        return remote(ref, ref, x_send.at[d, j], x_recv.at[d, j], ring_dev[d])

    def x_relay(j, d, lane):
        slot, q = arrival(j, d, x_parts, lane)
        ref = piece(x_h, slot, q)
        return remote(ref, ref, xp_send.at[d, j], xp_recv.at[d, j], partner)

    def x_wait(j, d):
        slot, q = arrival(j, d, x_parts, 0)
        ref = piece(x_h, slot, q)
        remote(ref, ref, x_send.at[d, j], x_recv.at[d, j], ring_dev[d]).wait_recv()

    def to_all(src, dst, sem):
        return [remote(src, dst, sem.at[0, d], sem.at[1, d], (me + d) % n) for d in range(1, n)]

    barrier = pltpu.get_barrier_semaphore()
    for d in range(1, n):
        pl.semaphore_signal(barrier, inc=1, device_id={'tp': (me + d) % n}, device_id_type=MESH)
    hid_copies = [pltpu.make_async_copy(hidden.at[pl.ds(t * TILE, TILE), :], hid.at[pl.ds(t * TILE, TILE), :], hid_sem.at[t]) for t in range(tiles)]
    for cp in hid_copies:
        cp.start()
    e_own = pltpu.make_async_copy(embed, e_all.at[me], loc_sem.at[0])
    e_own.start()
    pl.semaphore_wait(barrier, n - 1)

    tg_copies = to_all(tgt, tg_all.at[me], tg_sem)
    mk_copies = to_all(msk, mk_all.at[me], mk_sem)
    for cp in tg_copies + mk_copies:
        cp.start()
    for j in range(e_parts):
        for d in range(2):
            e_ring(j, d, embed).start()
    e_swap = remote(embed, e_all.at[me], e_pair.at[0], e_pair.at[1], partner)
    e_swap.start()

    tg_all[me] = tgt[...]
    mk_all[me] = msk[...]
    max_s[...] = jnp.full_like(max_s, -jnp.inf)
    sum_s[...] = jnp.zeros_like(sum_s)

    rows_ln = 64
    for t in range(tiles):
        hid_copies[t].wait()

        @pl.loop(0, TILE // rows_ln)
        def _(b):
            rows = pl.ds(pl.multiple_of(t * TILE + b * rows_ln, rows_ln), rows_ln)
            h = hid[rows, :].astype(F32)
            mu = jnp.mean(h, axis=-1, keepdims=True)
            cen = h - mu
            rs = lax.rsqrt(jnp.mean(cen * cen, axis=-1, keepdims=True) + LN_EPS)
            x_own[rows, :] = (cen * rs * gain[...] + bias[...]).astype(BF16)
            mu_s[rows, :] = jnp.broadcast_to(mu, (rows_ln, LANES))
            rs_s[rows, :] = jnp.broadcast_to(rs, (rows_ln, LANES))

    x_out = pltpu.make_async_copy(x_own, x_h.at[me], loc_sem.at[1])
    x_out.start()
    e_own.wait()

    def z_store(st, v):
        return pltpu.make_async_copy(zb.at[pl.ds(st * tiles, tiles)], z_h.at[v], z_sem.at[st])

    def stats(slot, q, st):
        e_piece = e_all[slot, pl.ds(pl.multiple_of(q * PIECE, PIECE), PIECE), :]
        half = tokens // 2
        for h in range(2):
            z = matmul_t(x_own[h * half:(h + 1) * half, :], e_piece)
            for b in range(half // TILE):
                zb[st * tiles + h * (half // TILE) + b] = z[b * TILE:(b + 1) * TILE, :]
        per = TILE // LANES
        for b in range(blocks):
            rows = slice(b * LANES, (b + 1) * LANES)
            z = zb[st * tiles + b // per, (b % per) * LANES:(b % per + 1) * LANES, :]
            z0, z1 = z[:, :LANES], z[:, LANES:]
            old = max_s[rows, :]
            new = jnp.maximum(old, jnp.maximum(z0, z1))
            sum_s[rows, :] = sum_s[rows, :] * jnp.exp(old - new) + jnp.exp(z0 - new) + jnp.exp(z1 - new)
            max_s[rows, :] = new

    @pl.loop(0, 2 * e_parts)
    def _(i):
        lane, q = i // e_parts, i % e_parts
        slot = me + lane * (1 - 2 * core)

        @pl.when(i == e_parts)
        def _():
            e_swap.wait_recv()

        @pl.when(i >= 2)
        def _():
            z_store(i % 2, 0).wait()
        stats(slot, q, i % 2)
        z_store(i % 2, slot * e_parts + q).start()

    x_out.wait()
    x_swap = remote(x_h.at[me], x_h.at[me], x_pair.at[0], x_pair.at[1], partner)
    x_swap.start()

    @pl.loop(0, e_rounds)
    def _(k):
        for d in range(2):
            e_wait(k, d)
        for d in range(2):
            e_relay(k, d, 0).start()

        @pl.when(k < e_parts // 2)
        def _():
            for d in range(2):
                e_ring(k + e_parts, d).start()

        @pl.when(k == e_parts // 2)
        def _():
            for j in range(2):
                for d in range(2):
                    x_ring(j, d).start()

        @pl.loop(0, 4)
        def _(i):
            lane, d = i // 2, i % 2

            @pl.when(i == 2)
            def _():
                for dd in range(2):
                    e_relay(k, dd, 1).wait_recv()
            slot, q = arrival(k, d, e_parts, lane)
            z_store(i % 2, 0).wait()
            stats(slot, q, i % 2)
            z_store(i % 2, slot * e_parts + q).start()

    for b in range(blocks):
        rows = slice(b * LANES, (b + 1) * LANES)
        part = max_s[rows, :]
        top = jnp.max(part, axis=-1, keepdims=True)
        tot = jnp.sum(sum_s[rows, :] * jnp.exp(part - top), axis=-1, keepdims=True)
        lse = jnp.broadcast_to(top + jnp.log(tot), (LANES, LANES))
        max_s[rows, :] = lse
        ls_all[me, b:b + 1, :] = jnp.transpose(lse)[0:1, :]
        sum_s[rows, :] = jnp.zeros((LANES, LANES), F32)
    for cp in mk_copies + tg_copies:
        cp.wait_recv()
    count = jnp.sum(jnp.sum(jnp.sum(mk_all[...].astype(F32), axis=0), axis=0, keepdims=True), axis=1, keepdims=True)
    inv_s[...] = jnp.broadcast_to(1.0 / count, inv_s.shape)
    for st in range(2):
        z_store(st, 0).wait()
    ls_copies = to_all(ls_all.at[me], ls_all.at[me], ls_sem)
    for cp in ls_copies:
        cp.start()

    chunks = n * shard // TILE
    halves = TILE // PIECE
    depth = 3

    def z_load(u, h):
        return pltpu.make_async_copy(z_h.at[(u % chunks) * halves + h, u // chunks], zb.at[(u % 4) * halves + h], zl_sem.at[u % 4, h])

    for u in range(depth):
        for h in range(halves):
            z_load(u, h).start()
    for j in range(2, x_parts):
        for d in range(2):
            x_ring(j, d).start()

    lane_ids = lax.broadcasted_iota(jnp.int32, (1, LANES), 1)

    def make_dz(t, vc, out):
        u = t * chunks + vc
        for h in range(halves):
            z_load(u, h).wait()

        @pl.when(u + depth < tiles * chunks)
        def _():
            for h in range(halves):
                z_load(u + depth, h).start()

        def work():
            slot = (u % 4) * halves
            for b in range(TILE // LANES):
                rows = slice(b * LANES, (b + 1) * LANES)
                tok = pl.ds(pl.multiple_of(t * TILE + b * LANES, LANES), LANES)
                lse, tc, wc = max_s[tok, :], tcol[rows, :], wcol[rows, :]
                found = sum_s[tok, :]
                for g in range(TILE // LANES):
                    lo = (g * LANES) % PIECE
                    z = zb[slot + g * LANES // PIECE, rows, lo:lo + LANES]
                    hit = tc == (lane_ids + (vc * TILE + g * LANES)).astype(F32)
                    p = jnp.exp(z - lse)
                    out[rows, g * LANES:(g + 1) * LANES] = (jnp.where(hit, p - 1.0, p) * wc).astype(BF16)
                    found = found + jnp.where(hit, z, 0.0)
                sum_s[tok, :] = found
        return work

    @pl.loop(0, tiles)
    def _(t):
        for b in range(TILE // LANES):
            row = pl.ds(t * (TILE // LANES) + b, 1)
            rows = slice(b * LANES, (b + 1) * LANES)
            tcol[rows, :] = to_col(tg_all[me, row, :].astype(F32))
            wcol[rows, :] = to_col(mk_all[me, row, :].astype(F32) * inv_s[0:1, :])
        dx_acc[...] = jnp.zeros_like(dx_acc)
        da = dz_a.at[pl.ds(0, TILE), :]
        db = dz_b.at[pl.ds(0, TILE), :]
        make_dz(t, 0, da)()

        @pl.loop(0, n - 1)
        def _(v):
            work = make_dz(t, 2 * v + 1, db)
            dx_acc[...] += matmul(da[...], e_all[v, 0:TILE, :])
            work()
            work = make_dz(t, 2 * v + 2, da)
            dx_acc[...] += matmul(db[...], e_all[v, TILE:2 * TILE, :])
            work()
        work = make_dz(t, chunks - 1, db)
        dx_acc[...] += matmul(da[...], e_all[n - 1, 0:TILE, :])
        work()
        dx_acc[...] += matmul(db[...], e_all[n - 1, TILE:2 * TILE, :])

        rows_bw = 32

        @pl.loop(0, TILE // rows_bw)
        def _(b):
            loc = pl.ds(pl.multiple_of(b * rows_bw, rows_bw), rows_bw)
            rows = pl.ds(pl.multiple_of(t * TILE + b * rows_bw, rows_bw), rows_bw)
            dx = dx_acc[loc, :]
            rs = widen(rs_s[rows, :], dim)
            xh = (hid[rows, :].astype(F32) - widen(mu_s[rows, :], dim)) * rs
            dxx = dx * xh

            @pl.when(t + b == 0)
            def _():
                gb[...] = jnp.zeros_like(gb)
            gb[0:8, :] += jnp.sum(dxx.reshape(rows_bw // 8, 8, dim), axis=0)
            gb[8:16, :] += jnp.sum(dx.reshape(rows_bw // 8, 8, dim), axis=0)
            g = dx * gain[...]
            c1 = jnp.mean(g, axis=-1, keepdims=True)
            c2 = jnp.mean(g * xh, axis=-1, keepdims=True)
            hid[rows, :] = (rs * (g - c1 - xh * c2)).astype(BF16)
        for b in range(TILE // LANES):
            row = pl.ds(t * (TILE // LANES) + b, 1)
            tok = pl.ds(pl.multiple_of(t * TILE + b * LANES, LANES), LANES)
            t_row = to_row(jnp.sum(sum_s[tok, :], axis=-1, keepdims=True))
            loss_o[row, :] = (ls_all[me, row, :] - t_row) * mk_all[me, row, :].astype(F32)
        out_rows = pl.ds(pl.multiple_of(t * TILE, TILE), TILE)
        pltpu.make_async_copy(hid.at[out_rows, :], dh_o.at[out_rows, :], dh_sem.at[t]).start()

    sm_all[me] = jnp.zeros(sm_all.shape[1:], F32)
    sm_all[me, 0:1, :] = jnp.sum(gb[0:8, :], axis=0, keepdims=True)
    sm_all[me, 1:2, :] = jnp.sum(gb[8:16, :], axis=0, keepdims=True)
    loss_sum = jnp.sum(jnp.sum(loss_o[...], axis=0, keepdims=True), axis=1, keepdims=True)
    sm_all[me, 2:3, :] = jnp.broadcast_to(loss_sum, (1, dim))

    de_acc[...] = jnp.zeros_like(de_acc)
    dz_b[...] = jnp.zeros_like(dz_b)
    xbuf[1, 1] = jnp.zeros(xbuf.shape[2:], BF16)
    for cp in ls_copies:
        cp.wait_recv()
    sm_copies = to_all(sm_all.at[me], sm_all.at[me], sm_sem)
    for cp in sm_copies:
        cp.start()
    x_swap.wait_recv()
    lead = x_parts // 2
    pairs = lead + x_rounds
    early = x_parts // 2

    def source(p, lane, d):
        far = (p + x_rounds) // pairs
        k = p - lead * far
        off = (2 * d - 1) * far * (1 + k // x_parts)
        side = core + lane * (1 - 2 * core)
        slot = 2 * ((chip + off + chips) % chips) + side
        q = far * ((k + d * (x_parts // 2)) % x_parts) + (1 - far) * (2 * p + d)
        return slot, q

    def x_load(p, lane, d):
        slot, q = source(p, lane, d)
        return pltpu.make_async_copy(piece(x_h, slot, q), xbuf.at[p % 2, lane, pl.ds(d * PIECE, PIECE), :], xl_sem.at[lane, d])

    base = me * shard

    def vocab_step(p, lane, dz_out, dz_in, xd):
        zt[...] = matmul_t(e_all[me], xbuf[p % 2, lane])
        de_acc[...] += matmul(dz_in[...], xd[...])
        cols = []
        for d in range(2):
            slot, q = source(p, lane, d)
            for r in range(PIECE // LANES):
                row = pl.ds(q * (PIECE // LANES) + r, 1)
                cols.append((ls_all[slot, row, :], tg_all[slot, row, :] - base, mk_all[slot, row, :].astype(F32) * inv_s[0:1, :]))
        ids = lax.broadcasted_iota(jnp.int32, (LANES, LANES), 0)
        for b in range(shard // LANES):
            rows = slice(b * LANES, (b + 1) * LANES)
            for g, (lse, tg, sc) in enumerate(cols):
                lanes = slice(g * LANES, (g + 1) * LANES)
                pr = jnp.exp(zt[rows, lanes] - lse)
                hit = ids == tg - b * LANES
                dz_out[rows, lanes] = (jnp.where(hit, pr - 1.0, pr) * sc).astype(BF16)

    for d in range(2):
        x_load(0, 0, d).start()

    @pl.loop(0, pairs)
    def _(p):
        @pl.when(p == 1)
        def _():
            for k in range(early):
                for d in range(2):
                    x_wait(k, d)
                for d in range(2):
                    x_ring(k + x_parts, d).start()
                for d in range(2):
                    x_relay(k, d, 0).start()

        @pl.when(p >= lead)
        def _():
            for d in range(2):
                x_relay(p - lead, d, 1).wait_recv()
        for d in range(2):
            x_load(p, 1, d).start()
        for d in range(2):
            x_load(p, 0, d).wait()
        vocab_step(p, 0, dz_a, dz_b, xbuf.at[1 - p % 2, 1])

        @pl.when(p + 1 >= lead + early)
        def _():
            @pl.when(p + 1 < pairs)
            def _():
                for d in range(2):
                    x_wait(p + 1 - lead, d)
                for d in range(2):
                    x_relay(p + 1 - lead, d, 0).start()

        @pl.when(p + 1 < pairs)
        def _():
            for d in range(2):
                x_load(p + 1, 0, d).start()
        for d in range(2):
            x_load(p, 1, d).wait()
        vocab_step(p, 1, dz_b, dz_a, xbuf.at[p % 2, 0])

    de_acc[...] += matmul(dz_b[...], xbuf[(pairs - 1) % 2, 1])
    de_out = pltpu.make_async_copy(de_acc, de_o, loc_sem.at[0])
    de_out.start()

    for cp in sm_copies:
        cp.wait_recv()
    total = sm_all[0]
    for r in range(1, n):
        total = total + sm_all[r]
    dg_o[...] = total[0:1, :]
    db_o[...] = total[1:2, :]
    mean_o[...] = total[2:3, 0:LANES] * inv_s[0:1, :]

    for cp in tg_copies + mk_copies + ls_copies + sm_copies:
        cp.wait_send()
    e_swap.wait_send()
    x_swap.wait_send()

    @pl.loop(0, e_rounds)
    def _(j):
        for d in range(2):
            e_ring(j, d).wait_send()
            e_relay(j, d, 0).wait_send()

    @pl.loop(0, x_rounds)
    def _(j):
        for d in range(2):
            x_ring(j, d).wait_send()
            x_relay(j, d, 0).wait_send()

    for t in range(tiles):
        rows = pl.ds(t * TILE, TILE)
        pltpu.make_async_copy(hid.at[rows, :], dh_o.at[rows, :], dh_sem.at[t]).wait()
    de_out.wait()


def solution(mesh):
    n = mesh.shape['tp']

    def body(hidden, ln_gain, ln_bias, embed, targets, loss_mask):
        tokens, dim = hidden.shape
        shard = embed.shape[0]
        blocks = tokens // LANES
        e_rounds = shard // PIECE * 3 // 2
        x_rounds = tokens // PIECE * 3 // 2
        tiles = tokens // TILE
        anywhere = pl.BlockSpec(memory_space=pl.ANY)
        vmem = pl.BlockSpec(memory_space=pltpu.VMEM)
        dma = pltpu.SemaphoreType.DMA
        sds = jax.ShapeDtypeStruct
        outs = pl.pallas_call(
            functools.partial(kernel, n),
            out_shape=(
                sds((blocks, LANES), F32), sds((1, LANES), F32), sds((tokens, dim), BF16), sds((shard, dim), F32),
                sds((1, dim), F32), sds((1, dim), F32),
                sds((n * shard // PIECE, tiles, TILE, PIECE), F32), sds((n, tokens, dim), BF16),
            ),
            in_specs=[anywhere, vmem, vmem, anywhere, vmem, vmem],
            out_specs=(vmem, vmem, anywhere, anywhere, vmem, vmem, anywhere, anywhere),
            scratch_shapes=[
                pltpu.VMEM((n, shard, dim), BF16), pltpu.VMEM((tokens, dim), BF16), pltpu.VMEM((tokens, dim), BF16),
                pltpu.VMEM((shard, dim), F32), pltpu.VMEM((tokens, LANES), F32), pltpu.VMEM((tokens, LANES), F32),
                pltpu.VMEM((tokens, LANES), F32), pltpu.VMEM((tokens, LANES), F32),
                pltpu.VMEM((2, 2, TILE, dim), BF16), pltpu.VMEM((shard, TILE), BF16), pltpu.VMEM((shard, TILE), BF16),
                pltpu.VMEM((8, TILE, PIECE), F32), pltpu.VMEM((TILE, dim), F32), pltpu.VMEM((shard, TILE), F32),
                pltpu.VMEM((TILE, LANES), F32), pltpu.VMEM((TILE, LANES), F32),
                pltpu.VMEM((n, blocks, LANES), jnp.int32), pltpu.VMEM((n, blocks, LANES), jnp.int32),
                pltpu.VMEM((n, blocks, LANES), F32), pltpu.VMEM((n, 8, dim), F32), pltpu.VMEM((16, dim), F32),
                pltpu.VMEM((8, LANES), F32),
                dma((2, e_rounds)), dma((2, e_rounds)), dma((2, e_rounds)), dma((2, e_rounds)), dma((2,)),
                dma((2, x_rounds)), dma((2, x_rounds)), dma((2, x_rounds)), dma((2, x_rounds)), dma((2,)),
                dma((2, n)), dma((2, n)), dma((2, n)), dma((2, n)),
                dma((tiles,)), dma((2,)), dma((2,)), dma((4, 2)), dma((2, 2)), dma((tiles,)),
            ],
            compiler_params=pltpu.CompilerParams(collective_id=0, has_side_effects=True, vmem_limit_bytes=60 * 1024 * 1024),
        )(hidden, ln_gain.reshape(1, dim), ln_bias.reshape(1, dim), embed, targets.reshape(blocks, LANES), loss_mask.reshape(blocks, LANES))
        loss, mean, d_hidden, d_embed, d_gain, d_bias = outs[:6]
        return loss.reshape(tokens), mean[0, :1], d_hidden, d_embed, d_gain.reshape(dim), d_bias.reshape(dim)

    rows = P(('dp', 'tp'))
    mat = P(('dp', 'tp'), None)
    return jax.shard_map(body, mesh=mesh, in_specs=(mat, P(), P(), P('tp', None), rows, rows), out_specs=(rows, P('dp'), mat, mat, P('dp'), P('dp')), check_vma=False)
```

```python
import functools

import jax
import jax.numpy as jnp
from jax import lax
from jax.experimental import pallas as pl
from jax.experimental.pallas import tpu as pltpu
from jax.sharding import PartitionSpec as P

LN_EPS = 1e-5
LANES = 128
PIECE = 256
TILE = 512
MESH = pl.DeviceIdType.MESH
F32 = jnp.float32
BF16 = jnp.bfloat16


def matmul_t(a, b):
    return lax.dot_general(a, b, (((1,), (1,)), ((), ())), preferred_element_type=F32)


def matmul(a, b):
    return jnp.dot(a, b, preferred_element_type=F32)


def widen(col, width):
    return jnp.concatenate([col] * (width // LANES), axis=1)


def to_row(col):
    return jnp.transpose(jnp.broadcast_to(col, (LANES, LANES)))[0:1, :]


def to_col(row):
    return jnp.transpose(jnp.broadcast_to(row, (LANES, LANES)))


def kernel(n, hidden, gain, bias, embed, tgt, msk,
           loss_o, mean_o, dh_o, de_o, dg_o, db_o, z_h, x_h, zt_h,
           e_all, x_own, hid, de_acc, max_s, sum_s, mu_s, rs_s, xbuf, dz_a, dz_b, zb, dx_0, dx_1, dh_0, dh_1, zt_0, zt_1,
           tcol, wcol, tg_all, mk_all, ls_all, sm_all, gb, inv_s,
           e_send, e_recv, ep_send, ep_recv, e_pair, x_send, x_recv, xp_send, xp_recv, x_pair,
           tg_sem, mk_sem, ls_sem, sm_sem, hid_sem, loc_sem, z_sem, zl_sem, xl_sem, dh_sem, zt_sem, xi_sem):
    tokens, dim = hid.shape
    shard = embed.shape[0]
    chips = n // 2
    e_parts, x_parts = shard // PIECE, tokens // PIECE
    e_rounds, x_rounds = e_parts + e_parts // 2, x_parts + x_parts // 2
    blocks = tokens // LANES
    tiles = tokens // TILE
    me = lax.axis_index('tp')
    chip, core = me // 2, me % 2
    partner = 2 * chip + 1 - core
    right, left = (me + 2) % n, (me + n - 2) % n
    ring_dev = (right, left)
    dxs, dhs, zts = (dx_0, dx_1), (dh_0, dh_1), (zt_0, zt_1)

    def remote(src, dst, ssem, rsem, dev):
        return pltpu.make_async_remote_copy(src_ref=src, dst_ref=dst, send_sem=ssem, recv_sem=rsem,
                                            device_id={'tp': dev}, device_id_type=MESH)

    def piece(buf, slot, q):
        return buf.at[slot, pl.ds(pl.multiple_of(q * PIECE, PIECE), PIECE), :]

    def ring_src(j, d, parts):
        off = (2 * d - 1) * (j // parts)
        return 2 * ((chip + off + chips) % chips) + core, (j + d * (parts // 2)) % parts

    def arrival(j, d, parts, lane):
        off = (2 * d - 1) * (1 + j // parts)
        side = core + lane * (1 - 2 * core)
        return 2 * ((chip + off + chips) % chips) + side, (j + d * (parts // 2)) % parts

    def e_ring(j, d, src=None):
        slot, q = ring_src(j, d, e_parts)
        ref = piece(e_all, slot, q)
        if src is None:
            src = ref
        else:
            src = src.at[pl.ds(pl.multiple_of(q * PIECE, PIECE), PIECE), :]
        return remote(src, ref, e_send.at[d, j], e_recv.at[d, j], ring_dev[d])

    def e_relay(j, d, lane):
        slot, q = arrival(j, d, e_parts, lane)
        ref = piece(e_all, slot, q)
        return remote(ref, ref, ep_send.at[d, j], ep_recv.at[d, j], partner)

    def e_wait(j, d):
        slot, q = arrival(j, d, e_parts, 0)
        ref = piece(e_all, slot, q)
        remote(ref, ref, e_send.at[d, j], e_recv.at[d, j], ring_dev[d]).wait_recv()

    def x_ring(j, d):
        slot, q = ring_src(j, d, x_parts)
        ref = piece(x_h, slot, q)
        return remote(ref, ref, x_send.at[d, j], x_recv.at[d, j], ring_dev[d])

    def x_relay(j, d, lane):
        slot, q = arrival(j, d, x_parts, lane)
        ref = piece(x_h, slot, q)
        return remote(ref, ref, xp_send.at[d, j], xp_recv.at[d, j], partner)

    def x_wait(j, d):
        slot, q = arrival(j, d, x_parts, 0)
        ref = piece(x_h, slot, q)
        remote(ref, ref, x_send.at[d, j], x_recv.at[d, j], ring_dev[d]).wait_recv()

    def to_all(src, dst, sem):
        return [remote(src, dst, sem.at[0, d], sem.at[1, d], (me + d) % n) for d in range(1, n)]

    barrier = pltpu.get_barrier_semaphore()
    for d in range(1, n):
        pl.semaphore_signal(barrier, inc=1, device_id={'tp': (me + d) % n}, device_id_type=MESH)
    hid_copies = [pltpu.make_async_copy(hidden.at[pl.ds(t * TILE, TILE), :], hid.at[pl.ds(t * TILE, TILE), :], hid_sem.at[t]) for t in range(tiles)]
    for cp in hid_copies:
        cp.start()
    e_own = pltpu.make_async_copy(embed, e_all.at[me], loc_sem.at[0])
    e_own.start()
    pl.semaphore_wait(barrier, n - 1)

    tg_copies = to_all(tgt, tg_all.at[me], tg_sem)
    mk_copies = to_all(msk, mk_all.at[me], mk_sem)
    for cp in tg_copies + mk_copies:
        cp.start()
    for j in range(e_parts):
        for d in range(2):
            e_ring(j, d, embed).start()
    e_swap = remote(embed, e_all.at[me], e_pair.at[0], e_pair.at[1], partner)
    e_swap.start()

    tg_all[me] = tgt[...]
    mk_all[me] = msk[...]
    max_s[...] = jnp.full_like(max_s, -jnp.inf)
    sum_s[...] = jnp.zeros_like(sum_s)

    rows_ln = 64
    for t in range(tiles):
        hid_copies[t].wait()

        @pl.loop(0, TILE // rows_ln)
        def _(b):
            rows = pl.ds(pl.multiple_of(t * TILE + b * rows_ln, rows_ln), rows_ln)
            h = hid[rows, :].astype(F32)
            mu = jnp.mean(h, axis=-1, keepdims=True)
            cen = h - mu
            rs = lax.rsqrt(jnp.mean(cen * cen, axis=-1, keepdims=True) + LN_EPS)
            x_own[rows, :] = (cen * rs * gain[...] + bias[...]).astype(BF16)
            mu_s[rows, :] = jnp.broadcast_to(mu, (rows_ln, LANES))
            rs_s[rows, :] = jnp.broadcast_to(rs, (rows_ln, LANES))

    x_out = pltpu.make_async_copy(x_own, x_h.at[me], loc_sem.at[1])
    x_out.start()
    e_own.wait()

    for cp in mk_copies + tg_copies:
        cp.wait_recv()
    count = jnp.sum(jnp.sum(jnp.sum(mk_all[...].astype(F32), axis=0), axis=0, keepdims=True), axis=1, keepdims=True)
    inv_s[...] = jnp.broadcast_to(1.0 / count, inv_s.shape)
    for b in range(blocks):
        rows = slice(b * LANES, (b + 1) * LANES)
        tcol[rows, :] = to_col(tgt[b:b + 1, :].astype(F32))
        wcol[rows, :] = to_col(msk[b:b + 1, :].astype(F32) * inv_s[0:1, :])

    def z_store(st, v):
        return pltpu.make_async_copy(zb.at[pl.ds(st * tiles, tiles)], z_h.at[v], z_sem.at[st])

    def stats(slot, q, st):
        e_piece = e_all[slot, pl.ds(pl.multiple_of(q * PIECE, PIECE), PIECE), :]
        half = tokens // 2
        for h in range(2):
            z = matmul_t(x_own[h * half:(h + 1) * half, :], e_piece)
            for b in range(half // TILE):
                zb[st * tiles + h * (half // TILE) + b] = z[b * TILE:(b + 1) * TILE, :]
        per = TILE // LANES
        for b in range(blocks):
            rows = slice(b * LANES, (b + 1) * LANES)
            z = zb[st * tiles + b // per, (b % per) * LANES:(b % per + 1) * LANES, :]
            z0, z1 = z[:, :LANES], z[:, LANES:]
            old = max_s[rows, :]
            new = jnp.maximum(old, jnp.maximum(z0, z1))
            sum_s[rows, :] = sum_s[rows, :] * jnp.exp(old - new) + jnp.exp(z0 - new) + jnp.exp(z1 - new)
            max_s[rows, :] = new

    @pl.loop(0, 2 * e_parts)
    def _(i):
        lane, q = i // e_parts, i % e_parts
        slot = me + lane * (1 - 2 * core)

        @pl.when(i == e_parts)
        def _():
            e_swap.wait_recv()

        @pl.when(i >= 2)
        def _():
            z_store(i % 2, 0).wait()
        stats(slot, q, i % 2)
        z_store(i % 2, slot * e_parts + q).start()

    x_out.wait()
    x_swap = remote(x_h.at[me], x_h.at[me], x_pair.at[0], x_pair.at[1], partner)
    x_swap.start()

    def zt_store(s, lane, t):
        return pltpu.make_async_copy(zts[s], zt_h.at[lane, t], zt_sem.at[s])

    def zt_load(lane, t):
        return pltpu.make_async_copy(zt_h.at[lane, t], zts[lane], zt_sem.at[lane])

    def near_load(s, lane, t):
        slot = me + lane * (1 - 2 * core)
        return pltpu.make_async_copy(x_h.at[slot, pl.ds(pl.multiple_of(t * TILE, TILE), TILE), :], xbuf.at[s, 0], xi_sem.at[s])

    @pl.loop(0, e_rounds)
    def _(k):
        for d in range(2):
            e_wait(k, d)
        for d in range(2):
            e_relay(k, d, 0).start()

        @pl.when(k < e_parts // 2)
        def _():
            for d in range(2):
                e_ring(k + e_parts, d).start()

        @pl.when(k == e_parts // 2)
        def _():
            for j in range(2):
                for d in range(2):
                    x_ring(j, d).start()

        @pl.loop(0, 4)
        def _(i):
            lane, d = i // 2, i % 2

            @pl.when(i == 2)
            def _():
                for dd in range(2):
                    e_relay(k, dd, 1).wait_recv()
            slot, q = arrival(k, d, e_parts, lane)
            z_store(i % 2, 0).wait()
            stats(slot, q, i % 2)
            z_store(i % 2, slot * e_parts + q).start()

        @pl.when(k == 1 + tiles // 2)
        def _():
            x_swap.wait_recv()

        @pl.when(k >= 1)
        def _():
            @pl.when(k <= tiles)
            def _():
                pos = 2 * (k - 1)
                for s in range(2):
                    near_load(s, (pos + s) // tiles, (pos + s) % tiles).start()
                for s in range(2):
                    near_load(s, 0, 0).wait()

                    @pl.when(k > 1)
                    def _():
                        zt_store(s, 0, 0).wait()
                    zts[s][...] = matmul_t(e_all[me], xbuf[s, 0])
                    zt_store(s, (pos + s) // tiles, (pos + s) % tiles).start()

    for b in range(blocks):
        rows = slice(b * LANES, (b + 1) * LANES)
        part = max_s[rows, :]
        top = jnp.max(part, axis=-1, keepdims=True)
        tot = jnp.sum(sum_s[rows, :] * jnp.exp(part - top), axis=-1, keepdims=True)
        lse = jnp.broadcast_to(top + jnp.log(tot), (LANES, LANES))
        max_s[rows, :] = lse
        ls_all[me, b:b + 1, :] = jnp.transpose(lse)[0:1, :]
        sum_s[rows, :] = jnp.zeros((LANES, LANES), F32)
    for st in range(2):
        z_store(st, 0).wait()
        zt_store(st, 0, 0).wait()
    ls_copies = to_all(ls_all.at[me], ls_all.at[me], ls_sem)
    for cp in ls_copies:
        cp.start()

    steps = tiles * n

    def z_load(u):
        return pltpu.make_async_copy(z_h.at[pl.ds((u % n) * e_parts, e_parts), (u // n) % tiles], zb.at[pl.ds((u % 2) * e_parts, e_parts)], zl_sem.at[u % 2])

    for u in range(2):
        z_load(u).start()
    for j in range(2, x_parts):
        for d in range(2):
            x_ring(j, d).start()

    lane_ids = lax.broadcasted_iota(jnp.int32, (1, LANES), 1)

    def make_dz(u, out):
        t, v = (u // n) % tiles, u % n
        slot = (u % 2) * e_parts
        for b in range(TILE // LANES):
            rows = slice(b * LANES, (b + 1) * LANES)
            tok = pl.ds(pl.multiple_of(t * TILE + b * LANES, LANES), LANES)
            lse, tc, wc = max_s[tok, :], tcol[tok, :], wcol[tok, :]
            found = sum_s[tok, :]
            for g in range(shard // LANES):
                lo = (g * LANES) % PIECE
                z = zb[slot + g * LANES // PIECE, rows, lo:lo + LANES]
                hit = tc == (lane_ids + (v * shard + g * LANES)).astype(F32)
                p = jnp.exp(z - lse)
                top, at = g * LANES // TILE * TILE + b * LANES, (g * LANES) % TILE
                out[top:top + LANES, at:at + LANES] = (jnp.where(hit, p - 1.0, p) * wc).astype(BF16)
                found = found + jnp.where(hit, z, 0.0)
            sum_s[tok, :] = found

    def norm_back(t, at, count_rows, dx_ref, dh_ref):
        step = 32
        for b in range(count_rows // step):
            loc = pl.ds(pl.multiple_of(at + b * step, step), step)
            rows = pl.ds(pl.multiple_of(t * TILE + at + b * step, step), step)
            dx = dx_ref[loc, :]
            dx_ref[loc, :] = jnp.zeros_like(dx)
            rs = widen(rs_s[rows, :], dim)
            xh = (hid[rows, :].astype(F32) - widen(mu_s[rows, :], dim)) * rs
            gb[0:8, :] += jnp.sum((dx * xh).reshape(step // 8, 8, dim), axis=0)
            gb[8:16, :] += jnp.sum(dx.reshape(step // 8, 8, dim), axis=0)
            g = dx * gain[...]
            c1 = jnp.mean(g, axis=-1, keepdims=True)
            c2 = jnp.mean(g * xh, axis=-1, keepdims=True)
            dh_ref[loc, :] = (rs * (g - c1 - xh * c2)).astype(BF16)

    def dh_out(t, s):
        return pltpu.make_async_copy(dhs[s], dh_o.at[pl.ds(pl.multiple_of(t * TILE, TILE), TILE), :], dh_sem.at[s])

    gb[...] = jnp.zeros_like(gb)
    for s in range(2):
        dxs[s][...] = jnp.zeros_like(dxs[s])
    z_load(0).wait()
    make_dz(0, dz_a)
    z_load(2).start()

    @pl.loop(0, tiles // 2)
    def _(tt):
        for s in range(2):
            t = 2 * tt + s
            prev = (t + tiles - 1) % tiles
            other = 1 - s

            @pl.when(t >= 3)
            def _():
                dh_out(0, other).wait()

            @pl.loop(0, n // 2)
            def _(w):
                for half, (now, later) in enumerate(((dz_a, dz_b), (dz_b, dz_a))):
                    v = 2 * w + half
                    u = t * n + v + 1
                    z_load(u).wait()
                    dxs[s][...] += matmul(now[0:TILE, :], e_all[v, 0:TILE, :]) + matmul(now[TILE:2 * TILE, :], e_all[v, TILE:2 * TILE, :])
                    make_dz(u, later)
                    norm_back(prev, v * (TILE // n), TILE // n, dxs[other], dhs[other])

                    @pl.when(u + 2 <= steps)
                    def _():
                        z_load(u + 2).start()

            @pl.when(t >= 1)
            def _():
                dh_out(prev, other).start()
            for b in range(TILE // LANES):
                row = pl.ds(t * (TILE // LANES) + b, 1)
                tok = pl.ds(pl.multiple_of(t * TILE + b * LANES, LANES), LANES)
                t_row = to_row(jnp.sum(sum_s[tok, :], axis=-1, keepdims=True))
                loss_o[row, :] = (ls_all[me, row, :] - t_row) * msk[row, :].astype(F32)

            for d in range(2):
                x_wait(t, d)
            for d in range(2):
                x_ring(t + x_parts, d).start()
            for d in range(2):
                x_relay(t, d, 0).start()

    last = (tiles - 1) % 2
    dh_out(0, last).wait()

    @pl.loop(0, n)
    def _(b):
        norm_back(tiles - 1, b * (TILE // n), TILE // n, dxs[last], dhs[last])
    dh_out(tiles - 1, last).start()

    sm_all[me] = jnp.zeros(sm_all.shape[1:], F32)
    sm_all[me, 0:1, :] = jnp.sum(gb[0:8, :], axis=0, keepdims=True)
    sm_all[me, 1:2, :] = jnp.sum(gb[8:16, :], axis=0, keepdims=True)
    loss_sum = jnp.sum(jnp.sum(loss_o[...], axis=0, keepdims=True), axis=1, keepdims=True)
    sm_all[me, 2:3, :] = jnp.broadcast_to(loss_sum, (1, dim))

    de_acc[...] = jnp.zeros_like(de_acc)
    dz_b[...] = jnp.zeros_like(dz_b)
    xbuf[1, 1] = jnp.zeros(xbuf.shape[2:], BF16)
    for cp in ls_copies:
        cp.wait_recv()
    sm_copies = to_all(sm_all.at[me], sm_all.at[me], sm_sem)
    for cp in sm_copies:
        cp.start()
    lead = x_parts // 2
    pairs = lead + x_rounds
    early = x_parts // 2

    def source(p, lane, d):
        far = (p + x_rounds) // pairs
        k = p - lead * far
        off = (2 * d - 1) * far * (1 + k // x_parts)
        side = core + lane * (1 - 2 * core)
        slot = 2 * ((chip + off + chips) % chips) + side
        q = far * ((k + d * (x_parts // 2)) % x_parts) + (1 - far) * (2 * p + d)
        return slot, q

    def x_load(p, lane, d):
        slot, q = source(p, lane, d)
        return pltpu.make_async_copy(piece(x_h, slot, q), xbuf.at[p % 2, lane, pl.ds(d * PIECE, PIECE), :], xl_sem.at[lane, d])

    base = me * shard

    def vocab_step(p, lane, dz_out, dz_in, xd, fresh):
        zt = zts[lane]
        if fresh:
            zt[...] = matmul_t(e_all[me], xbuf[p % 2, lane])
        de_acc[...] += matmul(dz_in[...], xd[...])
        cols = []
        for d in range(2):
            slot, q = source(p, lane, d)
            for r in range(PIECE // LANES):
                row = pl.ds(q * (PIECE // LANES) + r, 1)
                cols.append((ls_all[slot, row, :], tg_all[slot, row, :] - base, mk_all[slot, row, :].astype(F32) * inv_s[0:1, :]))
        ids = lax.broadcasted_iota(jnp.int32, (LANES, LANES), 0)
        for b in range(shard // LANES):
            rows = slice(b * LANES, (b + 1) * LANES)
            for g, (lse, tg, sc) in enumerate(cols):
                lanes = slice(g * LANES, (g + 1) * LANES)
                pr = jnp.exp(zt[rows, lanes] - lse)
                hit = ids == tg - b * LANES
                dz_out[rows, lanes] = (jnp.where(hit, pr - 1.0, pr) * sc).astype(BF16)

    for d in range(2):
        x_load(0, 0, d).start()
    for lane in range(2):
        zt_load(lane, 0).start()

    @pl.loop(0, lead)
    def _(p):
        for d in range(2):
            x_load(p, 1, d).start()
        for d in range(2):
            x_load(p, 0, d).wait()
        zt_load(0, 0).wait()
        vocab_step(p, 0, dz_a, dz_b, xbuf.at[1 - p % 2, 1], False)

        @pl.when(p + 1 < lead)
        def _():
            zt_load(0, p + 1).start()
        for d in range(2):
            x_load(p + 1, 0, d).start()
        for d in range(2):
            x_load(p, 1, d).wait()
        zt_load(1, 0).wait()
        vocab_step(p, 1, dz_b, dz_a, xbuf.at[p % 2, 0], False)

        @pl.when(p + 1 < lead)
        def _():
            zt_load(1, p + 1).start()

    @pl.loop(lead, pairs)
    def _(p):
        for d in range(2):
            x_relay(p - lead, d, 1).wait_recv()
        for d in range(2):
            x_load(p, 1, d).start()
        for d in range(2):
            x_load(p, 0, d).wait()
        vocab_step(p, 0, dz_a, dz_b, xbuf.at[1 - p % 2, 1], True)

        @pl.when(p + 1 < pairs)
        def _():
            @pl.when(p + 1 >= lead + early)
            def _():
                for d in range(2):
                    x_wait(p + 1 - lead, d)
                for d in range(2):
                    x_relay(p + 1 - lead, d, 0).start()
            for d in range(2):
                x_load(p + 1, 0, d).start()
        for d in range(2):
            x_load(p, 1, d).wait()
        vocab_step(p, 1, dz_b, dz_a, xbuf.at[p % 2, 0], True)

    de_acc[...] += matmul(dz_b[...], xbuf[(pairs - 1) % 2, 1])
    de_out = pltpu.make_async_copy(de_acc, de_o, loc_sem.at[0])
    de_out.start()

    for cp in sm_copies:
        cp.wait_recv()
    total = sm_all[0]
    for r in range(1, n):
        total = total + sm_all[r]
    dg_o[...] = total[0:1, :]
    db_o[...] = total[1:2, :]
    mean_o[...] = total[2:3, 0:LANES] * inv_s[0:1, :]

    for cp in tg_copies + mk_copies + ls_copies + sm_copies:
        cp.wait_send()
    e_swap.wait_send()
    x_swap.wait_send()

    @pl.loop(0, e_rounds)
    def _(j):
        for d in range(2):
            e_ring(j, d).wait_send()
            e_relay(j, d, 0).wait_send()

    @pl.loop(0, x_rounds)
    def _(j):
        for d in range(2):
            x_ring(j, d).wait_send()
            x_relay(j, d, 0).wait_send()

    for s in range(2):
        dh_out(0, s).wait()
    de_out.wait()


def solution(mesh):
    n = mesh.shape['tp']

    def body(hidden, ln_gain, ln_bias, embed, targets, loss_mask):
        tokens, dim = hidden.shape
        shard = embed.shape[0]
        blocks = tokens // LANES
        e_rounds = shard // PIECE * 3 // 2
        x_rounds = tokens // PIECE * 3 // 2
        tiles = tokens // TILE
        anywhere = pl.BlockSpec(memory_space=pl.ANY)
        vmem = pl.BlockSpec(memory_space=pltpu.VMEM)
        dma = pltpu.SemaphoreType.DMA
        sds = jax.ShapeDtypeStruct
        outs = pl.pallas_call(
            functools.partial(kernel, n),
            out_shape=(
                sds((blocks, LANES), F32), sds((1, LANES), F32), sds((tokens, dim), BF16), sds((shard, dim), F32),
                sds((1, dim), F32), sds((1, dim), F32),
                sds((n * shard // PIECE, tiles, TILE, PIECE), F32), sds((n, tokens, dim), BF16),
                sds((2, tiles, shard, TILE), F32),
            ),
            in_specs=[anywhere, vmem, vmem, anywhere, vmem, vmem],
            out_specs=(vmem, vmem, anywhere, anywhere, vmem, vmem, anywhere, anywhere, anywhere),
            scratch_shapes=[
                pltpu.VMEM((n, shard, dim), BF16), pltpu.VMEM((tokens, dim), BF16), pltpu.VMEM((tokens, dim), BF16),
                pltpu.VMEM((shard, dim), F32), pltpu.VMEM((tokens, LANES), F32), pltpu.VMEM((tokens, LANES), F32),
                pltpu.VMEM((tokens, LANES), F32), pltpu.VMEM((tokens, LANES), F32),
                pltpu.VMEM((2, 2, TILE, dim), BF16), pltpu.VMEM((shard, TILE), BF16), pltpu.VMEM((shard, TILE), BF16),
                pltpu.VMEM((8, TILE, PIECE), F32), pltpu.VMEM((TILE, dim), F32), pltpu.VMEM((TILE, dim), F32),
                pltpu.VMEM((TILE, dim), BF16), pltpu.VMEM((TILE, dim), BF16), pltpu.VMEM((shard, TILE), F32), pltpu.VMEM((shard, TILE), F32),
                pltpu.VMEM((tokens, LANES), F32), pltpu.VMEM((tokens, LANES), F32),
                pltpu.VMEM((n, blocks, LANES), jnp.int32), pltpu.VMEM((n, blocks, LANES), jnp.int32),
                pltpu.VMEM((n, blocks, LANES), F32), pltpu.VMEM((n, 8, dim), F32), pltpu.VMEM((16, dim), F32),
                pltpu.VMEM((8, LANES), F32),
                dma((2, e_rounds)), dma((2, e_rounds)), dma((2, e_rounds)), dma((2, e_rounds)), dma((2,)),
                dma((2, x_rounds)), dma((2, x_rounds)), dma((2, x_rounds)), dma((2, x_rounds)), dma((2,)),
                dma((2, n)), dma((2, n)), dma((2, n)), dma((2, n)),
                dma((tiles,)), dma((2,)), dma((2,)), dma((2,)), dma((2, 2)), dma((2,)), dma((2,)), dma((2,)),
            ],
            compiler_params=pltpu.CompilerParams(collective_id=0, has_side_effects=True, vmem_limit_bytes=63 * 1024 * 1024),
        )(hidden, ln_gain.reshape(1, dim), ln_bias.reshape(1, dim), embed, targets.reshape(blocks, LANES), loss_mask.reshape(blocks, LANES))
        loss, mean, d_hidden, d_embed, d_gain, d_bias = outs[:6]
        return loss.reshape(tokens), mean[0, :1], d_hidden, d_embed, d_gain.reshape(dim), d_bias.reshape(dim)

    rows = P(('dp', 'tp'))
    mat = P(('dp', 'tp'), None)
    return jax.shard_map(body, mesh=mesh, in_specs=(mat, P(), P(), P('tp', None), rows, rows), out_specs=(rows, P('dp'), mat, mat, P('dp'), P('dp')), check_vma=False)
```

```python
import functools

import jax
import jax.numpy as jnp
from jax import lax
from jax.experimental import pallas as pl
from jax.experimental.pallas import tpu as pltpu
from jax.sharding import PartitionSpec as P

LN_EPS = 1e-5
LANES = 128
PIECE = 256
TILE = 512
MESH = pl.DeviceIdType.MESH
F32 = jnp.float32
BF16 = jnp.bfloat16


def matmul_t(a, b):
    return lax.dot_general(a, b, (((1,), (1,)), ((), ())), preferred_element_type=F32)


def matmul(a, b):
    return jnp.dot(a, b, preferred_element_type=F32)


def widen(col, width):
    return jnp.concatenate([col] * (width // LANES), axis=1)


def to_row(col):
    return jnp.transpose(jnp.broadcast_to(col, (LANES, LANES)))[0:1, :]


def to_col(row):
    return jnp.transpose(jnp.broadcast_to(row, (LANES, LANES)))


def kernel(n, hidden, gain, bias, embed, tgt, msk,
           loss_o, mean_o, dh_o, de_o, dg_o, db_o, z_h, x_h, zt_h,
           e_all, x_own, hid, de_acc, max_s, sum_s, mu_s, rs_s, xbuf, dz_a, dz_b, zb, dx_0, dx_1, dh_0, dh_1, zt_0, zt_1,
           tcol, wcol, tg_all, mk_all, ls_all, sm_all, gb, inv_s,
           e_send, e_recv, ep_send, ep_recv, e_pair, x_send, x_recv, xp_send, xp_recv, x_pair,
           tg_sem, mk_sem, ls_sem, sm_sem, hid_sem, loc_sem, z_sem, zl_sem, xl_sem, dh_sem, zt_sem, xi_sem):
    tokens, dim = hid.shape
    shard = embed.shape[0]
    chips = n // 2
    e_parts, x_parts = shard // PIECE, tokens // PIECE
    e_rounds, x_rounds = e_parts + e_parts // 2, x_parts + x_parts // 2
    blocks = tokens // LANES
    tiles = tokens // TILE
    me = lax.axis_index('tp')
    chip, core = me // 2, me % 2
    partner = 2 * chip + 1 - core
    right, left = (me + 2) % n, (me + n - 2) % n
    ring_dev = (right, left)
    dxs, dhs, zts = (dx_0, dx_1), (dh_0, dh_1), (zt_0, zt_1)

    def remote(src, dst, ssem, rsem, dev):
        return pltpu.make_async_remote_copy(src_ref=src, dst_ref=dst, send_sem=ssem, recv_sem=rsem,
                                            device_id={'tp': dev}, device_id_type=MESH)

    def piece(buf, slot, q):
        return buf.at[slot, pl.ds(pl.multiple_of(q * PIECE, PIECE), PIECE), :]

    def ring_src(j, d, parts):
        off = (2 * d - 1) * (j // parts)
        return 2 * ((chip + off + chips) % chips) + core, (j + d * (parts // 2)) % parts

    def arrival(j, d, parts, lane):
        off = (2 * d - 1) * (1 + j // parts)
        side = core + lane * (1 - 2 * core)
        return 2 * ((chip + off + chips) % chips) + side, (j + d * (parts // 2)) % parts

    def e_ring(j, d, src=None):
        slot, q = ring_src(j, d, e_parts)
        ref = piece(e_all, slot, q)
        if src is None:
            src = ref
        else:
            src = src.at[pl.ds(pl.multiple_of(q * PIECE, PIECE), PIECE), :]
        return remote(src, ref, e_send.at[d, j], e_recv.at[d, j], ring_dev[d])

    def e_relay(j, d, lane):
        slot, q = arrival(j, d, e_parts, lane)
        ref = piece(e_all, slot, q)
        return remote(ref, ref, ep_send.at[d, j], ep_recv.at[d, j], partner)

    def e_wait(j, d):
        slot, q = arrival(j, d, e_parts, 0)
        ref = piece(e_all, slot, q)
        remote(ref, ref, e_send.at[d, j], e_recv.at[d, j], ring_dev[d]).wait_recv()

    def x_ring(j, d):
        slot, q = ring_src(j, d, x_parts)
        ref = piece(x_h, slot, q)
        return remote(ref, ref, x_send.at[d, j], x_recv.at[d, j], ring_dev[d])

    def x_relay(j, d, lane):
        slot, q = arrival(j, d, x_parts, lane)
        ref = piece(x_h, slot, q)
        return remote(ref, ref, xp_send.at[d, j], xp_recv.at[d, j], partner)

    def x_wait(j, d):
        slot, q = arrival(j, d, x_parts, 0)
        ref = piece(x_h, slot, q)
        remote(ref, ref, x_send.at[d, j], x_recv.at[d, j], ring_dev[d]).wait_recv()

    def to_all(src, dst, sem):
        return [remote(src, dst, sem.at[0, d], sem.at[1, d], (me + d) % n) for d in range(1, n)]

    barrier = pltpu.get_barrier_semaphore()
    for d in range(1, n):
        pl.semaphore_signal(barrier, inc=1, device_id={'tp': (me + d) % n}, device_id_type=MESH)
    hid_copies = [pltpu.make_async_copy(hidden.at[pl.ds(t * TILE, TILE), :], hid.at[pl.ds(t * TILE, TILE), :], hid_sem.at[t]) for t in range(tiles)]
    for cp in hid_copies:
        cp.start()
    e_own = pltpu.make_async_copy(embed, e_all.at[me], loc_sem.at[0])
    e_own.start()
    pl.semaphore_wait(barrier, n - 1)

    tg_copies = to_all(tgt, tg_all.at[me], tg_sem)
    mk_copies = to_all(msk, mk_all.at[me], mk_sem)
    for cp in tg_copies + mk_copies:
        cp.start()
    for j in range(e_parts):
        for d in range(2):
            e_ring(j, d, embed).start()
    e_swap = remote(embed, e_all.at[me], e_pair.at[0], e_pair.at[1], partner)
    e_swap.start()

    tg_all[me] = tgt[...]
    mk_all[me] = msk[...]
    max_s[...] = jnp.full_like(max_s, -jnp.inf)
    sum_s[...] = jnp.zeros_like(sum_s)

    rows_ln = 64
    for t in range(tiles):
        hid_copies[t].wait()

        @pl.loop(0, TILE // rows_ln)
        def _(b):
            rows = pl.ds(pl.multiple_of(t * TILE + b * rows_ln, rows_ln), rows_ln)
            h = hid[rows, :].astype(F32)
            mu = jnp.mean(h, axis=-1, keepdims=True)
            cen = h - mu
            rs = lax.rsqrt(jnp.mean(cen * cen, axis=-1, keepdims=True) + LN_EPS)
            x_own[rows, :] = (cen * rs * gain[...] + bias[...]).astype(BF16)
            mu_s[rows, :] = jnp.broadcast_to(mu, (rows_ln, LANES))
            rs_s[rows, :] = jnp.broadcast_to(rs, (rows_ln, LANES))

    x_out = pltpu.make_async_copy(x_own, x_h.at[me], loc_sem.at[1])
    x_out.start()
    e_own.wait()

    for cp in mk_copies + tg_copies:
        cp.wait_recv()
    count = jnp.sum(jnp.sum(jnp.sum(mk_all[...].astype(F32), axis=0), axis=0, keepdims=True), axis=1, keepdims=True)
    inv_s[...] = jnp.broadcast_to(1.0 / count, inv_s.shape)
    for b in range(blocks):
        rows = slice(b * LANES, (b + 1) * LANES)
        tcol[rows, :] = to_col(tgt[b:b + 1, :].astype(F32))
        wcol[rows, :] = to_col(msk[b:b + 1, :].astype(F32) * inv_s[0:1, :])

    def z_store(st, v):
        return pltpu.make_async_copy(zb.at[pl.ds(st * tiles, tiles)], z_h.at[v], z_sem.at[st])

    def stats(slot, q, st):
        e_piece = e_all[slot, pl.ds(pl.multiple_of(q * PIECE, PIECE), PIECE), :]
        half = tokens // 2
        for h in range(2):
            z = matmul_t(x_own[h * half:(h + 1) * half, :], e_piece)
            for b in range(half // TILE):
                zb[st * tiles + h * (half // TILE) + b] = z[b * TILE:(b + 1) * TILE, :]
        per = TILE // LANES
        for b in range(blocks):
            rows = slice(b * LANES, (b + 1) * LANES)
            z = zb[st * tiles + b // per, (b % per) * LANES:(b % per + 1) * LANES, :]
            z0, z1 = z[:, :LANES], z[:, LANES:]
            old = max_s[rows, :]
            new = jnp.maximum(old, jnp.maximum(z0, z1))
            sum_s[rows, :] = sum_s[rows, :] * jnp.exp(old - new) + jnp.exp(z0 - new) + jnp.exp(z1 - new)
            max_s[rows, :] = new

    @pl.loop(0, 2 * e_parts)
    def _(i):
        lane, q = i // e_parts, i % e_parts
        slot = me + lane * (1 - 2 * core)

        @pl.when(i == e_parts)
        def _():
            e_swap.wait_recv()

        @pl.when(i >= 2)
        def _():
            z_store(i % 2, 0).wait()
        stats(slot, q, i % 2)
        z_store(i % 2, slot * e_parts + q).start()

    x_out.wait()
    x_swap = remote(x_h.at[me], x_h.at[me], x_pair.at[0], x_pair.at[1], partner)
    x_swap.start()

    def zt_store(s, lane, t):
        return pltpu.make_async_copy(zts[s], zt_h.at[lane, t], zt_sem.at[s])

    def zt_load(lane, t):
        return pltpu.make_async_copy(zt_h.at[lane, t], zts[lane], zt_sem.at[lane])

    def near_load(s, lane, t):
        slot = me + lane * (1 - 2 * core)
        return pltpu.make_async_copy(x_h.at[slot, pl.ds(pl.multiple_of(t * TILE, TILE), TILE), :], xbuf.at[s, 0], xi_sem.at[s])

    @pl.loop(0, e_rounds)
    def _(k):
        for d in range(2):
            e_wait(k, d)
        for d in range(2):
            e_relay(k, d, 0).start()

        @pl.when(k < e_parts // 2)
        def _():
            for d in range(2):
                e_ring(k + e_parts, d).start()

        @pl.when(k == e_parts // 2)
        def _():
            for j in range(2):
                for d in range(2):
                    x_ring(j, d).start()

        @pl.loop(0, 4)
        def _(i):
            lane, d = i // 2, i % 2

            @pl.when(i == 2)
            def _():
                for dd in range(2):
                    e_relay(k, dd, 1).wait_recv()
            slot, q = arrival(k, d, e_parts, lane)
            z_store(i % 2, 0).wait()
            stats(slot, q, i % 2)
            z_store(i % 2, slot * e_parts + q).start()

        @pl.when(k == 1 + tiles // 2)
        def _():
            x_swap.wait_recv()

        @pl.when(k >= 1)
        def _():
            @pl.when(k <= tiles)
            def _():
                pos = 2 * (k - 1)
                for s in range(2):
                    near_load(s, (pos + s) // tiles, (pos + s) % tiles).start()
                for s in range(2):
                    near_load(s, 0, 0).wait()

                    @pl.when(k > 1)
                    def _():
                        zt_store(s, 0, 0).wait()
                    zts[s][...] = matmul_t(e_all[me], xbuf[s, 0])
                    zt_store(s, (pos + s) // tiles, (pos + s) % tiles).start()

    for b in range(blocks):
        rows = slice(b * LANES, (b + 1) * LANES)
        part = max_s[rows, :]
        top = jnp.max(part, axis=-1, keepdims=True)
        tot = jnp.sum(sum_s[rows, :] * jnp.exp(part - top), axis=-1, keepdims=True)
        lse = jnp.broadcast_to(top + jnp.log(tot), (LANES, LANES))
        max_s[rows, :] = lse
        ls_all[me, b:b + 1, :] = jnp.transpose(lse)[0:1, :]
        sum_s[rows, :] = jnp.zeros((LANES, LANES), F32)
    for st in range(2):
        z_store(st, 0).wait()
        zt_store(st, 0, 0).wait()
    ls_copies = to_all(ls_all.at[me], ls_all.at[me], ls_sem)
    for cp in ls_copies:
        cp.start()

    steps = tiles * n

    def z_load(u):
        return pltpu.make_async_copy(z_h.at[pl.ds((u % n) * e_parts, e_parts), (u // n) % tiles], zb.at[pl.ds((u % 2) * e_parts, e_parts)], zl_sem.at[u % 2])

    for u in range(2):
        z_load(u).start()
    for j in range(2, x_parts):
        for d in range(2):
            x_ring(j, d).start()

    lane_ids = lax.broadcasted_iota(jnp.int32, (1, LANES), 1)

    def make_dz(u, out):
        t, v = (u // n) % tiles, u % n
        slot = (u % 2) * e_parts
        for b in range(TILE // LANES):
            rows = slice(b * LANES, (b + 1) * LANES)
            tok = pl.ds(pl.multiple_of(t * TILE + b * LANES, LANES), LANES)
            lse, tc, wc = max_s[tok, :], tcol[tok, :], wcol[tok, :]
            found = sum_s[tok, :]
            for g in range(shard // LANES):
                lo = (g * LANES) % PIECE
                z = zb[slot + g * LANES // PIECE, rows, lo:lo + LANES]
                hit = tc == (lane_ids + (v * shard + g * LANES)).astype(F32)
                p = jnp.exp(z - lse)
                top, at = g * LANES // TILE * TILE + b * LANES, (g * LANES) % TILE
                out[top:top + LANES, at:at + LANES] = (jnp.where(hit, p - 1.0, p) * wc).astype(BF16)
                found = jnp.where(hit, z, found)
            sum_s[tok, :] = found

    def norm_back(t, at, count_rows, dx_ref, dh_ref):
        step = 32
        for b in range(count_rows // step):
            loc = pl.ds(pl.multiple_of(at + b * step, step), step)
            rows = pl.ds(pl.multiple_of(t * TILE + at + b * step, step), step)
            dx = dx_ref[loc, :]
            dx_ref[loc, :] = jnp.zeros_like(dx)
            rs = widen(rs_s[rows, :], dim)
            xh = (hid[rows, :].astype(F32) - widen(mu_s[rows, :], dim)) * rs
            gb[0:8, :] += jnp.sum((dx * xh).reshape(step // 8, 8, dim), axis=0)
            gb[8:16, :] += jnp.sum(dx.reshape(step // 8, 8, dim), axis=0)
            g = dx * gain[...]
            c1 = jnp.mean(g, axis=-1, keepdims=True)
            c2 = jnp.mean(g * xh, axis=-1, keepdims=True)
            dh_ref[loc, :] = (rs * (g - c1 - xh * c2)).astype(BF16)

    def dh_out(t, s):
        return pltpu.make_async_copy(dhs[s], dh_o.at[pl.ds(pl.multiple_of(t * TILE, TILE), TILE), :], dh_sem.at[s])

    gb[...] = jnp.zeros_like(gb)
    for s in range(2):
        dxs[s][...] = jnp.zeros_like(dxs[s])
    z_load(0).wait()
    make_dz(0, dz_a)
    z_load(2).start()

    @pl.loop(0, tiles // 2)
    def _(tt):
        for s in range(2):
            t = 2 * tt + s
            prev = (t + tiles - 1) % tiles
            other = 1 - s

            @pl.when(t >= 3)
            def _():
                dh_out(0, other).wait()

            @pl.loop(0, n // 2)
            def _(w):
                for half, (now, later) in enumerate(((dz_a, dz_b), (dz_b, dz_a))):
                    v = 2 * w + half
                    u = t * n + v + 1
                    z_load(u).wait()
                    dxs[s][...] += matmul(now[0:TILE, :], e_all[v, 0:TILE, :]) + matmul(now[TILE:2 * TILE, :], e_all[v, TILE:2 * TILE, :])
                    make_dz(u, later)
                    norm_back(prev, v * (TILE // n), TILE // n, dxs[other], dhs[other])

                    @pl.when(u + 2 <= steps)
                    def _():
                        z_load(u + 2).start()

            @pl.when(t >= 1)
            def _():
                dh_out(prev, other).start()
            for b in range(TILE // LANES):
                row = pl.ds(t * (TILE // LANES) + b, 1)
                tok = pl.ds(pl.multiple_of(t * TILE + b * LANES, LANES), LANES)
                t_row = to_row(jnp.sum(sum_s[tok, :], axis=-1, keepdims=True))
                loss_o[row, :] = (ls_all[me, row, :] - t_row) * msk[row, :].astype(F32)

            for d in range(2):
                x_wait(t, d)
            for d in range(2):
                x_ring(t + x_parts, d).start()
            for d in range(2):
                x_relay(t, d, 0).start()

    last = (tiles - 1) % 2
    dh_out(0, last).wait()

    @pl.loop(0, n)
    def _(b):
        norm_back(tiles - 1, b * (TILE // n), TILE // n, dxs[last], dhs[last])
    dh_out(tiles - 1, last).start()

    sm_all[me] = jnp.zeros(sm_all.shape[1:], F32)
    sm_all[me, 0:1, :] = jnp.sum(gb[0:8, :], axis=0, keepdims=True)
    sm_all[me, 1:2, :] = jnp.sum(gb[8:16, :], axis=0, keepdims=True)
    loss_sum = jnp.sum(jnp.sum(loss_o[...], axis=0, keepdims=True), axis=1, keepdims=True)
    sm_all[me, 2:3, :] = jnp.broadcast_to(loss_sum, (1, dim))

    de_acc[...] = jnp.zeros_like(de_acc)
    dz_b[...] = jnp.zeros_like(dz_b)
    xbuf[1, 1] = jnp.zeros(xbuf.shape[2:], BF16)
    for cp in ls_copies:
        cp.wait_recv()
    sm_copies = to_all(sm_all.at[me], sm_all.at[me], sm_sem)
    for cp in sm_copies:
        cp.start()
    lead = x_parts // 2
    pairs = lead + x_rounds
    early = x_parts // 2

    def source(p, lane, d):
        far = (p + x_rounds) // pairs
        k = p - lead * far
        off = (2 * d - 1) * far * (1 + k // x_parts)
        side = core + lane * (1 - 2 * core)
        slot = 2 * ((chip + off + chips) % chips) + side
        q = far * ((k + d * (x_parts // 2)) % x_parts) + (1 - far) * (2 * p + d)
        return slot, q

    def x_load(p, lane, d):
        slot, q = source(p, lane, d)
        return pltpu.make_async_copy(piece(x_h, slot, q), xbuf.at[p % 2, lane, pl.ds(d * PIECE, PIECE), :], xl_sem.at[lane, d])

    base = me * shard

    def vocab_step(p, lane, dz_out, dz_in, xd, fresh):
        zt = zts[lane]
        if fresh:
            zt[...] = matmul_t(e_all[me], xbuf[p % 2, lane])
        de_acc[...] += matmul(dz_in[...], xd[...])
        cols = []
        for d in range(2):
            slot, q = source(p, lane, d)
            for r in range(PIECE // LANES):
                row = pl.ds(q * (PIECE // LANES) + r, 1)
                cols.append((ls_all[slot, row, :], tg_all[slot, row, :] - base, mk_all[slot, row, :].astype(F32) * inv_s[0:1, :]))
        ids = lax.broadcasted_iota(jnp.int32, (LANES, LANES), 0)
        for b in range(shard // LANES):
            rows = slice(b * LANES, (b + 1) * LANES)
            for g, (lse, tg, sc) in enumerate(cols):
                lanes = slice(g * LANES, (g + 1) * LANES)
                pr = jnp.exp(zt[rows, lanes] - lse)
                hit = ids == tg - b * LANES
                dz_out[rows, lanes] = (jnp.where(hit, pr - 1.0, pr) * sc).astype(BF16)

    for d in range(2):
        x_load(0, 0, d).start()
    for lane in range(2):
        zt_load(lane, 0).start()

    @pl.loop(0, lead)
    def _(p):
        for d in range(2):
            x_load(p, 1, d).start()
        for d in range(2):
            x_load(p, 0, d).wait()
        zt_load(0, 0).wait()
        vocab_step(p, 0, dz_a, dz_b, xbuf.at[1 - p % 2, 1], False)

        @pl.when(p + 1 < lead)
        def _():
            zt_load(0, p + 1).start()
        for d in range(2):
            x_load(p + 1, 0, d).start()
        for d in range(2):
            x_load(p, 1, d).wait()
        zt_load(1, 0).wait()
        vocab_step(p, 1, dz_b, dz_a, xbuf.at[p % 2, 0], False)

        @pl.when(p + 1 < lead)
        def _():
            zt_load(1, p + 1).start()

    @pl.loop(lead, pairs)
    def _(p):
        for d in range(2):
            x_relay(p - lead, d, 1).wait_recv()
        for d in range(2):
            x_load(p, 1, d).start()
        for d in range(2):
            x_load(p, 0, d).wait()
        vocab_step(p, 0, dz_a, dz_b, xbuf.at[1 - p % 2, 1], True)

        @pl.when(p + 1 < pairs)
        def _():
            @pl.when(p + 1 >= lead + early)
            def _():
                for d in range(2):
                    x_wait(p + 1 - lead, d)
                for d in range(2):
                    x_relay(p + 1 - lead, d, 0).start()
            for d in range(2):
                x_load(p + 1, 0, d).start()
        for d in range(2):
            x_load(p, 1, d).wait()
        vocab_step(p, 1, dz_b, dz_a, xbuf.at[p % 2, 0], True)

    de_acc[...] += matmul(dz_b[...], xbuf[(pairs - 1) % 2, 1])
    de_out = pltpu.make_async_copy(de_acc, de_o, loc_sem.at[0])
    de_out.start()

    for cp in sm_copies:
        cp.wait_recv()
    total = sm_all[0]
    for r in range(1, n):
        total = total + sm_all[r]
    dg_o[...] = total[0:1, :]
    db_o[...] = total[1:2, :]
    mean_o[...] = total[2:3, 0:LANES] * inv_s[0:1, :]

    for cp in tg_copies + mk_copies + ls_copies + sm_copies:
        cp.wait_send()
    e_swap.wait_send()
    x_swap.wait_send()

    @pl.loop(0, e_rounds)
    def _(j):
        for d in range(2):
            e_ring(j, d).wait_send()
            e_relay(j, d, 0).wait_send()

    @pl.loop(0, x_rounds)
    def _(j):
        for d in range(2):
            x_ring(j, d).wait_send()
            x_relay(j, d, 0).wait_send()

    for s in range(2):
        dh_out(0, s).wait()
    de_out.wait()


def solution(mesh):
    n = mesh.shape['tp']

    def body(hidden, ln_gain, ln_bias, embed, targets, loss_mask):
        tokens, dim = hidden.shape
        shard = embed.shape[0]
        blocks = tokens // LANES
        e_rounds = shard // PIECE * 3 // 2
        x_rounds = tokens // PIECE * 3 // 2
        tiles = tokens // TILE
        anywhere = pl.BlockSpec(memory_space=pl.ANY)
        vmem = pl.BlockSpec(memory_space=pltpu.VMEM)
        dma = pltpu.SemaphoreType.DMA
        sds = jax.ShapeDtypeStruct
        outs = pl.pallas_call(
            functools.partial(kernel, n),
            out_shape=(
                sds((blocks, LANES), F32), sds((1, LANES), F32), sds((tokens, dim), BF16), sds((shard, dim), F32),
                sds((1, dim), F32), sds((1, dim), F32),
                sds((n * shard // PIECE, tiles, TILE, PIECE), F32), sds((n, tokens, dim), BF16),
                sds((2, tiles, shard, TILE), F32),
            ),
            in_specs=[anywhere, vmem, vmem, anywhere, vmem, vmem],
            out_specs=(vmem, vmem, anywhere, anywhere, vmem, vmem, anywhere, anywhere, anywhere),
            scratch_shapes=[
                pltpu.VMEM((n, shard, dim), BF16), pltpu.VMEM((tokens, dim), BF16), pltpu.VMEM((tokens, dim), BF16),
                pltpu.VMEM((shard, dim), F32), pltpu.VMEM((tokens, LANES), F32), pltpu.VMEM((tokens, LANES), F32),
                pltpu.VMEM((tokens, LANES), F32), pltpu.VMEM((tokens, LANES), F32),
                pltpu.VMEM((2, 2, TILE, dim), BF16), pltpu.VMEM((shard, TILE), BF16), pltpu.VMEM((shard, TILE), BF16),
                pltpu.VMEM((8, TILE, PIECE), F32), pltpu.VMEM((TILE, dim), F32), pltpu.VMEM((TILE, dim), F32),
                pltpu.VMEM((TILE, dim), BF16), pltpu.VMEM((TILE, dim), BF16), pltpu.VMEM((shard, TILE), F32), pltpu.VMEM((shard, TILE), F32),
                pltpu.VMEM((tokens, LANES), F32), pltpu.VMEM((tokens, LANES), F32),
                pltpu.VMEM((n, blocks, LANES), jnp.int32), pltpu.VMEM((n, blocks, LANES), jnp.int32),
                pltpu.VMEM((n, blocks, LANES), F32), pltpu.VMEM((n, 8, dim), F32), pltpu.VMEM((16, dim), F32),
                pltpu.VMEM((8, LANES), F32),
                dma((2, e_rounds)), dma((2, e_rounds)), dma((2, e_rounds)), dma((2, e_rounds)), dma((2,)),
                dma((2, x_rounds)), dma((2, x_rounds)), dma((2, x_rounds)), dma((2, x_rounds)), dma((2,)),
                dma((2, n)), dma((2, n)), dma((2, n)), dma((2, n)),
                dma((tiles,)), dma((2,)), dma((2,)), dma((2,)), dma((2, 2)), dma((2,)), dma((2,)), dma((2,)),
            ],
            compiler_params=pltpu.CompilerParams(collective_id=0, has_side_effects=True, vmem_limit_bytes=63 * 1024 * 1024),
        )(hidden, ln_gain.reshape(1, dim), ln_bias.reshape(1, dim), embed, targets.reshape(blocks, LANES), loss_mask.reshape(blocks, LANES))
        loss, mean, d_hidden, d_embed, d_gain, d_bias = outs[:6]
        return loss.reshape(tokens), mean[0, :1], d_hidden, d_embed, d_gain.reshape(dim), d_bias.reshape(dim)

    rows = P(('dp', 'tp'))
    mat = P(('dp', 'tp'), None)
    return jax.shard_map(body, mesh=mesh, in_specs=(mat, P(), P(), P('tp', None), rows, rows), out_specs=(rows, P('dp'), mat, mat, P('dp'), P('dp')), check_vma=False)
```
